32 devices in a mesh: groups: 2 (over x), gx: 8 (over z, y), gy: 2 (over core).
Axes of the slice: x: 2, y: 2, z: 4, core: 2. Of those that a mesh axis runs over, the one named last changes fastest.
Arguments:
- source: float32 [2, 3, 2, 32, 64, 256], P('groups', None, None, 'gx', 'gy'), parts along dimension 0, may hold values from -12 to 12
- permittivity: float32 [6, 32, 64, 256], P('groups', 'gx', 'gy'), parts along dimension 0, may hold values from 1 to 12
- frequency: float32 [1], replicated, may hold values from 0.25 to 0.6
Outputs:
- solution: float32 [2, 3, 2, 32, 64, 256], P('groups', None, None, 'gx', 'gy'), parts along dimension 0
- residual: float32 [2, 3, 2, 32, 64, 256], P('groups', None, None, 'gx', 'gy'), parts along dimension 0
The draws below stay inside these ranges and needn't reach their ends.
There are 2 independent parts, one for each index of `groups`. The reference program is written for one: setup_inputs(seed, part) draws one part's arguments, and reference() takes and returns one part's arrays. A program takes and returns all parts, laid end to end along the dimension named above; an argument that names none is the same for every part. Nothing has to cross between parts.
All inputs are finite; a program needn't handle non-finite values.
Results may differ from the reference program's by a relative error of at most 0.0003.
Values sent between devices are 32-bit elements; how exact they have to be, the bound alone decides.
A program may use at most 64 MiB of HBM per device.

```python
import jax
import jax.numpy as jnp

WAVES = 1
NZ = 256
PML = 8
ITERS = 3
NX = 32
NY = 64


def draw_source(key, part):
    noise_key = jax.random.fold_in(jax.random.fold_in(key, 17), 0)
    target = (WAVES, 3, 2, NX, NY, NZ)
    place_x = jnp.arange(NX, dtype=jnp.int32).astype(jnp.float32) / max(NX - 1, 1)
    rising = (1.0 + 2.0 * place_x).reshape(1, 1, 1, NX, 1, 1)
    return (jax.random.truncated_normal(noise_key, -4.0, 4.0, target, jnp.float32) * rising).astype(jnp.float32)


def steps_of(rng, extent, shards, smallest, top_value):
    def one(axis_at, parts):
        steps = jax.random.uniform(jax.random.fold_in(jax.random.fold_in(rng, 6), axis_at), (parts,), jnp.float32, smallest / len(shards), top_value / len(shards))
        return jnp.repeat(jnp.exp(steps), extent[axis_at] // parts).reshape((-1,) + (1,) * (len(extent) - axis_at - 1))

    factor_of = one(*shards[0])
    for cut in shards[1:]:
        factor_of = factor_of * one(*cut)
    return factor_of


def setup_inputs(seed: int = 0, part: int = 0) -> dict:
    splits = jax.random.split(jax.random.key(seed), 4)
    part_keys = jax.random.split(jax.random.fold_in(splits[3], part), 4)
    source = draw_source(jax.random.fold_in(jax.random.fold_in(splits[3], part), 71), part)
    permittivity = jnp.clip(1.0 + 11.0 * jax.random.uniform(part_keys[1], (3, NX, NY, NZ), jnp.float32) ** steps_of(part_keys[1], (3, NX, NY, NZ), ((1, 8), (2, 2)), -0.2, 0.2), 1.0, 12.0)
    frequency = jnp.clip(jax.random.uniform(splits[2], (WAVES,), jnp.float32, 0.25, 0.6), 0.25, 0.6)
    return {"source": source, "permittivity": permittivity, "frequency": frequency}


pml_strength = 2.0


def stretch(points, length, frequency):
    inside = jnp.maximum(jnp.maximum(PML - points, points - (length - PML)), 0.0) / PML
    damping = pml_strength * inside ** 3 / frequency[:, None]
    factor = 1.0 / (1.0 + damping * damping)
    return jnp.stack([factor, -damping * factor], axis=1)


def orient(coefficient, dimension):
    target = [coefficient.shape[0], 2, 1, 1, 1]
    target[dimension] = coefficient.shape[2]
    return coefficient.reshape(target)


def times_coef(values, coefficient):
    real_part = values[:, 0] * coefficient[:, 0] - values[:, 1] * coefficient[:, 1]
    imag_part = values[:, 0] * coefficient[:, 1] + values[:, 1] * coefficient[:, 0]
    return jnp.stack([real_part, imag_part], axis=1)


def curl_forward(extended, front_x, front_y, front_z):
    centre = extended[:, :, :, :-1, :-1]

    def step_x(component):
        return extended[:, component, :, 1:, :-1] - centre[:, component]

    def step_y(component):
        return extended[:, component, :, :-1, 1:] - centre[:, component]

    def step_z(component):
        cells = centre[:, component]
        above = jnp.concatenate([cells[..., 1:], jnp.zeros_like(cells[..., :1])], axis=-1)
        return above - cells

    curl_x = times_coef(step_y(2), front_y) - times_coef(step_z(1), front_z)
    curl_y = times_coef(step_z(0), front_z) - times_coef(step_x(2), front_x)
    curl_z = times_coef(step_x(1), front_x) - times_coef(step_y(0), front_y)
    return jnp.stack([curl_x, curl_y, curl_z], axis=1)


def curl_backward(padded, back_x, back_y, back_z):
    centre = padded[:, :, :, 1:, 1:]

    def step_x(component):
        return centre[:, component] - padded[:, component, :, :-1, 1:]

    def step_y(component):
        return centre[:, component] - padded[:, component, :, 1:, :-1]

    def step_z(component):
        cells = centre[:, component]
        below = jnp.concatenate([jnp.zeros_like(cells[..., :1]), cells[..., :-1]], axis=-1)
        return cells - below

    out_x = times_coef(step_y(2), back_y) - times_coef(step_z(1), back_z)
    out_y = times_coef(step_z(0), back_z) - times_coef(step_x(2), back_x)
    out_z = times_coef(step_x(1), back_x) - times_coef(step_y(0), back_y)
    return jnp.stack([out_x, out_y, out_z], axis=1)


def scaled(values, number):
    real_scale = number[0].reshape(-1, 1, 1, 1, 1)
    imag_scale = number[1].reshape(-1, 1, 1, 1, 1)
    real_part = values[:, :, 0] * real_scale - values[:, :, 1] * imag_scale
    imag_part = values[:, :, 0] * imag_scale + values[:, :, 1] * real_scale
    return jnp.stack([real_part, imag_part], axis=2)


def product(left, right):
    real_part = jnp.sum(left[:, :, 0] * right[:, :, 0] + left[:, :, 1] * right[:, :, 1], axis=(1, 2, 3, 4))
    imag_part = jnp.sum(left[:, :, 0] * right[:, :, 1] - left[:, :, 1] * right[:, :, 0], axis=(1, 2, 3, 4))
    return jnp.stack([real_part, imag_part])


def complex_times(first, other):
    return jnp.stack([first[0] * other[0] - first[1] * other[1], first[0] * other[1] + first[1] * other[0]])


def complex_ratio(first, other):
    modulus = other[0] * other[0] + other[1] * other[1]
    return jnp.stack([first[0] * other[0] + first[1] * other[1], first[1] * other[0] - first[0] * other[1]]) / modulus


def grid_factors(length, frequency, dimension):
    points = jnp.arange(length, dtype=jnp.int32).astype(jnp.float32)
    front = orient(stretch(points + 0.5, length, frequency), dimension)
    back = orient(stretch(points, length, frequency), dimension)
    return front, back


def reference(source, permittivity, frequency):
    front_x, back_x = grid_factors(NX, frequency, 2)
    front_y, back_y = grid_factors(NY, frequency, 3)
    front_z, back_z = grid_factors(NZ, frequency, 4)

    def operate(values):
        extended = jnp.pad(values, ((0, 0), (0, 0), (0, 0), (0, 1), (0, 1), (0, 0)))
        rotated = curl_forward(extended, front_x, front_y, front_z)
        padded = jnp.pad(rotated, ((0, 0), (0, 0), (0, 0), (1, 0), (1, 0), (0, 0)))
        applied = curl_backward(padded, back_x, back_y, back_z)
        return applied - (frequency * frequency).reshape(-1, 1, 1, 1, 1, 1) * permittivity[None, :, None] * values

    solution = jnp.zeros_like(source)
    residual = source
    shadow = source
    direction = source
    shadow_dot = product(shadow, residual)
    for iteration in range(ITERS):
        applied = operate(direction)
        step_size = complex_ratio(shadow_dot, product(shadow, applied))
        middle = residual - scaled(applied, step_size)
        second = operate(middle)
        weight = complex_ratio(product(second, middle), product(second, second))
        solution = solution + scaled(direction, step_size) + scaled(middle, weight)
        residual = middle - scaled(second, weight)
        if iteration + 1 < ITERS:
            shadow_next = product(shadow, residual)
            momentum = complex_times(complex_ratio(shadow_next, shadow_dot), complex_ratio(step_size, weight))
            direction = residual + scaled(direction - scaled(applied, weight), momentum)
            shadow_dot = shadow_next
    return solution, residual
```

```python
import functools

import jax
import jax.numpy as jnp
from jax import lax
from jax.experimental import pallas as pl
from jax.experimental.pallas import tpu as pltpu
from jax.sharding import PartitionSpec as P

PML = 8
ITERS = 3
STEPS = 2 * ITERS
SLOTS = 8
CENTRE = 4.0
HALF = 8.0
LANES = 128
pml_strength = 2.0

DOWN, UP, Y_DOWN, Y_UP, DIAG_DOWN, DIAG_UP = range(6)


def stretch(points, length, frequency):
    inside = jnp.maximum(jnp.maximum(PML - points, points - (length - PML)), 0.0) / PML
    damping = pml_strength * inside * inside * inside / frequency
    factor = 1.0 / (1.0 + damping * damping)
    return factor, -damping * factor


def cmul(a, b):
    return a[0] * b[0] - a[1] * b[1], a[0] * b[1] + a[1] * b[0]


def cadd(a, b):
    return a[0] + b[0], a[1] + b[1]


def csub(a, b):
    return a[0] - b[0], a[1] - b[1]


def cdiv(a, b):
    modulus = b[0] * b[0] + b[1] * b[1]
    return (a[0] * b[0] + a[1] * b[1]) / modulus, (a[1] * b[0] - a[0] * b[1]) / modulus


def kernel(sizes, src, eps, freq, x_out, r_out, V, mat, H, recv_e, recv_p, send_p, recv_yd,
           recv_yu, send_yd, send_yu, recv_dd, recv_du, send_dd, send_du, hrow, fxt, bxt, fyt,
           byt, fym, fzt, bzt, gram, send_g, recv_g, coef, send_sem, recv_sem, gsend_sem,
           grecv_sem, local_sem):
    gx_n, gy_n = sizes
    X, Y, Z = V.shape[3:]
    gx, gy = lax.axis_index("gx"), lax.axis_index("gy")
    frequency = freq[0]
    first_x, last_x = gx == 0, gx == gx_n - 1
    first_y, last_y = gy == 0, gy == gy_n - 1
    devices = gx_n * gy_n
    me = gx * gy_n + gy

    load_src = pltpu.make_async_copy(src, V.at[0], local_sem.at[0])
    load_eps = pltpu.make_async_copy(eps, mat, local_sem.at[1])
    load_src.start()
    load_eps.start()

    barrier = pltpu.get_barrier_semaphore()

    def greet(d, carry):
        other = lax.rem(me + d, devices)
        pl.semaphore_signal(
            barrier, inc=1, device_id={"gx": other // gy_n, "gy": lax.rem(other, gy_n)},
            device_id_type=pl.DeviceIdType.MESH)
        return carry

    lax.fori_loop(1, devices, greet, 0)

    def fill(ref, pair):
        ref[0] = pair[0]
        ref[1] = pair[1]

    def iota(shape, dim):
        return lax.broadcasted_iota(jnp.int32, shape, dim)

    rows_x = fxt.shape[1]
    px = (gx * X - 1 + iota((rows_x, Z), 0)).astype(jnp.float32) + 0.5
    front = stretch(px, X * gx_n, frequency)
    keep = jnp.logical_or(iota((rows_x, Z), 0) > 0, jnp.full((rows_x, Z), gx, jnp.int32) > 0)
    fill(fxt, [jnp.where(keep, f, 0.0) for f in front])
    px = (gx * X + iota((rows_x, Z), 0)).astype(jnp.float32)
    fill(bxt, stretch(px, X * gx_n, frequency))
    py = (gy * Y + iota((Y, Z), 0)).astype(jnp.float32)
    fill(fyt, stretch(py + 0.5, Y * gy_n, frequency))
    fill(byt, stretch(py, Y * gy_n, frequency))
    pm = (gy * Y - 1 + iota((8, Z), 0)).astype(jnp.float32) + 0.5
    keep = jnp.full((8, Z), gy, jnp.int32) > 0
    fill(fym, [jnp.where(keep, f, 0.0) for f in stretch(pm, Y * gy_n, frequency)])
    pz = iota((8, Z), 1).astype(jnp.float32)
    fill(fzt, stretch(pz + 0.5, Z, frequency))
    fill(bzt, stretch(pz, Z, frequency))

    @pl.when(last_x)
    def _():
        recv_e[...] = jnp.zeros_like(recv_e)

    @pl.when(first_x)
    def _():
        recv_p[...] = jnp.zeros_like(recv_p)

    @pl.when(last_y)
    def _():
        recv_yd[...] = jnp.zeros_like(recv_yd)

    @pl.when(first_y)
    def _():
        recv_yu[...] = jnp.zeros_like(recv_yu)

    @pl.when(jnp.logical_or(last_x, first_y))
    def _():
        recv_dd[...] = jnp.zeros_like(recv_dd)

    @pl.when(jnp.logical_or(first_x, last_y))
    def _():
        recv_du[...] = jnp.zeros_like(recv_du)

    gram[...] = jnp.zeros_like(gram)

    def copy(kind, k, source, target, dx, dy):
        return pltpu.make_async_remote_copy(
            src_ref=source, dst_ref=target, send_sem=send_sem.at[kind, k],
            recv_sem=recv_sem.at[kind, k], device_id={"gx": gx + dx, "gy": gy + dy},
            device_id_type=pl.DeviceIdType.MESH)

    def messages(k):
        return {
            DOWN: (lambda: copy(DOWN, k, V.at[k, 1:3, :, 0], recv_e.at[k], -1, 0),
                   gx > 0, gx < gx_n - 1),
            UP: (lambda: copy(UP, k, send_p.at[k], recv_p.at[k], 1, 0),
                 gx < gx_n - 1, gx > 0),
            Y_DOWN: (lambda: copy(Y_DOWN, k, send_yd.at[k], recv_yd.at[k], 0, -1),
                     gy > 0, gy < gy_n - 1),
            Y_UP: (lambda: copy(Y_UP, k, send_yu.at[k], recv_yu.at[k], 0, 1),
                   gy < gy_n - 1, gy > 0),
            DIAG_DOWN: (lambda: copy(DIAG_DOWN, k, send_dd.at[k], recv_dd.at[k], -1, 1),
                        jnp.logical_and(gx > 0, gy < gy_n - 1),
                        jnp.logical_and(gx < gx_n - 1, gy > 0)),
            DIAG_UP: (lambda: copy(DIAG_UP, k, send_du.at[k], recv_du.at[k], 1, -1),
                      jnp.logical_and(gx < gx_n - 1, gy > 0),
                      jnp.logical_and(gx > 0, gy < gy_n - 1)),
        }

    def send(k, kind):
        message, sends, _ = messages(k)[kind]
        pl.when(sends)(lambda: message().start())

    def receive(k, kind):
        message, _, receives = messages(k)[kind]
        pl.when(receives)(lambda: message().wait_recv())

    def row(ref, index):
        return ref[0, pl.ds(index, 1)], ref[1, pl.ds(index, 1)]

    def whole(ref):
        return ref[0], ref[1]

    def next_z(values):
        rolled = pltpu.roll(values, Z - 1, 1)
        return jnp.where(iota(values.shape, 1) == Z - 1, 0.0, rolled)

    def prev_z(values):
        rolled = pltpu.roll(values, 1, 1)
        return jnp.where(iota(values.shape, 1) == 0, 0.0, rolled)

    def next_y(values, edge):
        rolled = pltpu.roll(values, Y - 1, 0)
        return jnp.where(iota(values.shape, 0) == Y - 1, edge, rolled)

    def prev_y(values, edge):
        rolled = pltpu.roll(values, 1, 0)
        return jnp.where(iota(values.shape, 0) == 0, edge, rolled)

    def both(f, *pairs):
        return tuple(f(*[p[i] for p in pairs]) for i in range(2))

    def front_dz(pair):
        return cmul(both(lambda a: next_z(a) - a, pair), row(fzt, 0))

    def back_dz(pair):
        return cmul(both(lambda a: a - prev_z(a), pair), row(bzt, 0))

    def cell(k, component, x):
        return V[k, component, 0, x], V[k, component, 1, x]

    def cells_at(k, component, y):
        return V[k, component, 0, :, y, :], V[k, component, 1, :, y, :]

    zero_row = jnp.zeros((1, Z), jnp.float32)

    def dots(k):
        def one(j, carry):
            re = jnp.zeros((Y, Z), jnp.float32)
            im = jnp.zeros((Y, Z), jnp.float32)
            for component in range(3):
                for x in range(X):
                    a, b = cell(j, component, x), cell(k, component, x)
                    re = re + (a[0] * b[0] + a[1] * b[1])
                    im = im + (a[0] * b[1] - a[1] * b[0])

            def fold(values):
                values = jnp.sum(values, axis=0, keepdims=True)
                return sum(values[:, i:i + LANES] for i in range(0, Z, LANES))

            re, im = fold(re), fold(im)
            gram[pl.ds(j * SLOTS + k, 1)] = re
            gram[pl.ds(k * SLOTS + j, 1)] = re
            gram[pl.ds((SLOTS + j) * SLOTS + k, 1)] = im
            gram[pl.ds((SLOTS + k) * SLOTS + j, 1)] = -im
            return carry

        lax.fori_loop(0, k + 1, one, 0)

    def h_layer(k, x, above_y, above_z):
        ex, ey, ez = cell(k, 0, x), cell(k, 1, x), cell(k, 2, x)
        fx, fy = row(fxt, x + 1), whole(fyt)
        ez_edge = recv_yd[k, 1, 0, pl.ds(x, 1)], recv_yd[k, 1, 1, pl.ds(x, 1)]
        ex_edge = recv_yd[k, 0, 0, pl.ds(x, 1)], recv_yd[k, 0, 1, pl.ds(x, 1)]

        def dy(pair, edge):
            return cmul(both(lambda a, e: next_y(a, e) - a, pair, edge), fy)

        hx = csub(dy(ez, ez_edge), front_dz(ey))
        hy = csub(front_dz(ex), cmul(csub(above_z, ez), fx))
        hz = csub(cmul(csub(above_y, ey), fx), dy(ex, ex_edge))
        for component, pair in enumerate((hx, hy, hz)):
            for part in range(2):
                H[component, part, x] = pair[part]

    def hcell(component, x):
        return H[component, 0, x], H[component, 1, x]

    def out_layer(k, x, below_y, below_z, a_k, b_k):
        hx, hy, hz = hcell(0, x), hcell(1, x), hcell(2, x)
        bx, by = row(bxt, x), whole(byt)
        hx_edge = hrow[0, 0, pl.ds(x, 1)], hrow[0, 1, pl.ds(x, 1)]
        hz_edge = hrow[1, 0, pl.ds(x, 1)], hrow[1, 1, pl.ds(x, 1)]

        def dy(pair, edge):
            return cmul(both(lambda a, e: a - prev_y(a, e), pair, edge), by)

        cx = csub(dy(hz, hz_edge), back_dz(hy))
        cy = csub(back_dz(hx), cmul(csub(hz, below_z), bx))
        cz = csub(cmul(csub(hy, below_y), bx), dy(hx, hx_edge))
        before = jnp.maximum(k - 1, 0)
        for component, pair in enumerate((cx, cy, cz)):
            material = mat[component, x]
            for part in range(2):
                value = a_k * (pair[part] - material * V[k, component, part, x])
                V[k + 1, component, part, x] = value - b_k * V[before, component, part, x]

    def step(k, carry):
        a_k = jnp.where(k == 0, 1.0 / HALF, 2.0 / HALF).astype(jnp.float32)
        b_k = jnp.where(k == 0, 0.0, 1.0).astype(jnp.float32)
        top = X - 1

        for part in range(2):
            send_dd[k, pl.ds(part, 1)] = V[k, 1, part, 0, pl.ds(Y - 1, 1)]
            send_du[k, pl.ds(part, 1)] = V[k, 0, part, top, pl.ds(0, 1)]
            for i, component in enumerate((0, 2)):
                for x in range(X):
                    send_yd[k, i, part, pl.ds(x, 1)] = V[k, component, part, x, pl.ds(0, 1)]
        send(k, DIAG_DOWN)
        send(k, DIAG_UP)
        send(k, Y_DOWN)
        send(k, DOWN)

        ex, ey, ez = cell(k, 0, top), cell(k, 1, top), cell(k, 2, top)
        fx = row(fxt, X)
        fy = whole(fyt)
        py_ = cadd(front_dz(ex), cmul(ez, fx))
        dy = cmul(both(lambda a: next_y(a, zero_row) - a, ex), fy)
        pz_ = cadd(cmul(ey, fx), dy)
        for part in range(2):
            send_p[k, 0, part] = py_[part]
            send_p[k, 1, part] = -pz_[part]
        send(k, UP)

        fy = row(fyt, Y - 1)
        for x in range(X):
            at = pl.ds(Y - 1, 1)
            ex, ey, ez = ((V[k, c, 0, x, at], V[k, c, 1, x, at]) for c in range(3))
            if x < top:
                ahead = V[k, 1, 0, x + 1, at], V[k, 1, 1, x + 1, at]
            else:
                ahead = zero_row, zero_row
            qx = cadd(cmul(ez, fy), front_dz(ey))
            qz = cadd(cmul(csub(ahead, ey), row(fxt, x + 1)), cmul(ex, fy))
            for part in range(2):
                send_yu[k, 0, part, pl.ds(x, 1)] = -qx[part]
                send_yu[k, 1, part, pl.ds(x, 1)] = qz[part]
        send(k, Y_UP)

        receive(k, Y_DOWN)
        for x in range(X - 1):
            h_layer(k, x, cell(k, 1, x + 1), cell(k, 2, x + 1))

        receive(k, Y_UP)
        fm = row(fym, 0)
        for x in range(X):
            at = pl.ds(0, 1)
            ex, ez = ((V[k, c, 0, x, at], V[k, c, 1, x, at]) for c in (0, 2))
            qx = recv_yu[k, 0, 0, pl.ds(x, 1)], recv_yu[k, 0, 1, pl.ds(x, 1)]
            qz = recv_yu[k, 1, 0, pl.ds(x, 1)], recv_yu[k, 1, 1, pl.ds(x, 1)]
            hx, hz = cadd(qx, cmul(ez, fm)), csub(qz, cmul(ex, fm))
            for part in range(2):
                hrow[0, part, pl.ds(x, 1)] = hx[part]
                hrow[1, part, pl.ds(x, 1)] = hz[part]
        for x in range(1, X - 1):
            out_layer(k, x, hcell(1, x - 1), hcell(2, x - 1), a_k, b_k)

        dots(k)

        receive(k, DIAG_DOWN)
        fix = cmul((recv_dd[k, pl.ds(0, 1)], recv_dd[k, pl.ds(1, 1)]), row(fxt, X))
        for part in range(2):
            hrow[1, part, pl.ds(top, 1)] = hrow[1, part, pl.ds(top, 1)] + fix[part]
        receive(k, DOWN)
        h_layer(k, top, (recv_e[k, 0, 0], recv_e[k, 0, 1]), (recv_e[k, 1, 0], recv_e[k, 1, 1]))
        out_layer(k, top, hcell(1, top - 1), hcell(2, top - 1), a_k, b_k)

        receive(k, DIAG_UP)
        receive(k, UP)
        fx = row(fxt, 0)
        hy = csub((recv_p[k, 0, 0], recv_p[k, 0, 1]), cmul(cell(k, 2, 0), fx))
        hz = cadd((recv_p[k, 1, 0], recv_p[k, 1, 1]), cmul(cell(k, 1, 0), fx))
        fix = cmul((recv_du[k, pl.ds(0, 1)], recv_du[k, pl.ds(1, 1)]), row(fyt, Y - 1))
        hz = both(lambda a, f: jnp.where(iota((Y, Z), 0) == Y - 1, a - f, a), hz, fix)
        out_layer(k, 0, hy, hz, a_k, b_k)
        return carry

    load_eps.wait()
    square = frequency * frequency
    for component in range(3):
        for x in range(X):
            mat[component, x] = mat[component, x] * square + CENTRE
    load_src.wait()
    pl.semaphore_wait(barrier, devices - 1)

    lax.fori_loop(0, STEPS, step, 0)
    dots(STEPS)

    sums = jnp.sum(gram[...], axis=1, keepdims=True)
    count = 2 * SLOTS * SLOTS
    spread = jnp.where(iota((count, LANES), 0) == iota((count, LANES), 1), sums, 0.0)
    send_g[...] = jnp.sum(spread, axis=0, keepdims=True)
    recv_g[me] = send_g[...]

    def gram_copy(d, slot):
        other = lax.rem(me + d, devices)
        return pltpu.make_async_remote_copy(
            src_ref=send_g, dst_ref=recv_g.at[slot], send_sem=gsend_sem.at[d],
            recv_sem=grecv_sem.at[slot],
            device_id={"gx": other // gy_n, "gy": lax.rem(other, gy_n)},
            device_id_type=pl.DeviceIdType.MESH)

    def start(d, carry):
        gram_copy(d, me).start()
        return carry

    lax.fori_loop(1, devices, start, 0)

    def finish(d, carry):
        gram_copy(d, lax.rem(me + d, devices)).wait_recv()
        return carry

    lax.fori_loop(1, devices, finish, 0)
    total = jnp.broadcast_to(jnp.sum(recv_g[...], axis=0), (SLOTS, LANES))

    tile = (SLOTS, LANES)
    sub, lane = iota(tile, 0), iota(tile, 1)

    def unpack(start_at):
        out = jnp.zeros(tile, jnp.float32)
        for i in range(SLOTS):
            shift = (LANES - start_at - i * SLOTS) % LANES
            moved = total if shift == 0 else pltpu.roll(total, shift, 1)
            out = jnp.where(sub == i, moved, out)
        return jnp.where(lane < SLOTS, out, 0.0)

    g = unpack(0), unpack(SLOTS * SLOTS)

    def combine(f, *vectors):
        return tuple(f(*[v[i] for v in vectors]) for i in range(2))

    def operate(vector):
        def one(axis, index, size):
            lift = jnp.where(index == 1, 1.0, jnp.where(index == 0, 0.0, 0.5))
            drop = jnp.where(index < SLOTS - 1, 0.5, 0.0)

            def real(p):
                moved = lift * pltpu.roll(p, 1, axis) + drop * pltpu.roll(p, size - 1, axis)
                return CENTRE * p + HALF * moved
            return real

        along, down = vector
        return (both(one(1, lane, LANES), along), both(one(0, sub, SLOTS), down))

    def inner(left, right):
        t = cmul(g, right[0])
        a = left[1]

        def full(values):
            return jnp.sum(jnp.sum(values, axis=1, keepdims=True), axis=0, keepdims=True)

        return full(a[0] * t[0] + a[1] * t[1]), full(a[0] * t[1] - a[1] * t[0])

    def scaled(vector, number):
        return combine(lambda v: cmul(v, number), vector)

    zero = jnp.zeros(tile, jnp.float32)
    unit = ((jnp.where(lane == 0, 1.0, 0.0), zero), (jnp.where(sub == 0, 1.0, 0.0), zero))
    answer = ((zero, zero), (zero, zero))
    residual = direction = unit
    rho = inner(unit, unit)
    for iteration in range(ITERS):
        image = operate(direction)
        alpha = cdiv(rho, inner(unit, image))
        middle = combine(csub, residual, scaled(image, alpha))
        second = operate(middle)
        weight = cdiv(inner(second, middle), inner(second, second))
        answer = combine(cadd, answer, scaled(direction, alpha))
        answer = combine(cadd, answer, scaled(middle, weight))
        residual = combine(csub, middle, scaled(second, weight))
        if iteration + 1 < ITERS:
            moved = cmul(weight, inner(unit, second))
            rho_next = -moved[0], -moved[1]
            beta = cmul(cdiv(rho_next, rho), cdiv(alpha, weight))
            pull = combine(csub, direction, scaled(image, weight))
            direction = combine(cadd, residual, scaled(pull, beta))
            rho = rho_next

    for i, values in enumerate((answer[1][0], answer[1][1], residual[1][0], residual[1][1])):
        for at in range(0, Z, LANES):
            coef[i, :, pl.ds(at, LANES)] = values

    def emit(index, carry):
        component = index // X
        x = lax.rem(index, X)
        for out, base, last in ((x_out, 0, STEPS), (r_out, 2, STEPS + 1)):
            re = im = jnp.zeros((Y, Z), jnp.float32)
            for k in range(last):
                c = coef[base, pl.ds(k, 1)], coef[base + 1, pl.ds(k, 1)]
                v = V[k, component, 0, x], V[k, component, 1, x]
                p = cmul(v, c)
                re, im = re + p[0], im + p[1]
            out[component, 0, x] = re
            out[component, 1, x] = im
        return carry

    lax.fori_loop(0, 3 * X, emit, 0)

    def drain(k, carry):
        for message, sends, _ in messages(k).values():
            pl.when(sends)(lambda: message().wait_send())
        return carry

    lax.fori_loop(0, STEPS, drain, 0)

    def drain_gram(d, carry):
        gram_copy(d, me).wait_send()
        return carry

    lax.fori_loop(1, devices, drain_gram, 0)


def solution(mesh):
    gx_n, gy_n = mesh.shape["gx"], mesh.shape["gy"]
    devices = gx_n * gy_n

    def body(source, permittivity, frequency):
        X, Y, Z = source.shape[3:]
        field = source.shape[1:]
        f32 = jnp.float32
        rows_x = -(-(X + 1) // 8) * 8
        vmem = pltpu.VMEM
        face = (STEPS, 2, 2, Y, Z)
        rows = (STEPS, 2, 2, X, Z)
        diag = (STEPS, 2, Z)
        scratch = [
            vmem((STEPS + 1,) + field, f32), vmem(permittivity.shape, f32), vmem(field, f32),
            vmem(face, f32), vmem(face, f32), vmem(face, f32),
            vmem(rows, f32), vmem(rows, f32), vmem(rows, f32), vmem(rows, f32),
            vmem(diag, f32), vmem(diag, f32), vmem(diag, f32), vmem(diag, f32),
            vmem(rows[1:], f32),
            vmem((2, rows_x, Z), f32), vmem((2, rows_x, Z), f32),
            vmem((2, Y, Z), f32), vmem((2, Y, Z), f32), vmem((2, 8, Z), f32),
            vmem((2, 8, Z), f32), vmem((2, 8, Z), f32),
            vmem((2 * SLOTS * SLOTS, LANES), f32), vmem((1, LANES), f32),
            vmem((devices, 1, LANES), f32), vmem((4, SLOTS, Z), f32),
            pltpu.SemaphoreType.DMA((6, STEPS)), pltpu.SemaphoreType.DMA((6, STEPS)),
            pltpu.SemaphoreType.DMA((devices,)), pltpu.SemaphoreType.DMA((devices,)),
            pltpu.SemaphoreType.DMA((2,)),
        ]
        out = pl.pallas_call(
            functools.partial(kernel, (gx_n, gy_n)),
            out_shape=(jax.ShapeDtypeStruct(field, f32),) * 2,
            in_specs=[pl.BlockSpec(memory_space=pl.ANY), pl.BlockSpec(memory_space=pl.ANY),
                      pl.BlockSpec(memory_space=pltpu.SMEM)],
            out_specs=(pl.BlockSpec(memory_space=vmem),) * 2,
            scratch_shapes=scratch,
            compiler_params=pltpu.CompilerParams(
                collective_id=0, has_side_effects=True, vmem_limit_bytes=48 * 1024 * 1024),
        )(source[0], permittivity, frequency)
        return out[0][None], out[1][None]

    placed = (P("groups", None, None, "gx", "gy", None), P("groups", "gx", "gy", None), P())
    return jax.shard_map(
        body,
        mesh=mesh,
        in_specs=placed,
        out_specs=(
            P("groups", None, None, "gx", "gy", None),
            P("groups", None, None, "gx", "gy", None),
        ),
        check_vma=False,
    )
```

```python
import functools

import jax
import jax.numpy as jnp
from jax import lax
from jax.experimental import pallas as pl
from jax.experimental.pallas import tpu as pltpu
from jax.sharding import PartitionSpec as P

PML = 8
ITERS = 3
STEPS = 2 * ITERS
SLOTS = 8
CENTRE = 4.0
HALF = 8.0
LANES = 128
pml_strength = 2.0

DOWN, UP, Y_DOWN, Y_UP, DIAG_DOWN, DIAG_UP = range(6)


def stretch(points, length, frequency):
    inside = jnp.maximum(jnp.maximum(PML - points, points - (length - PML)), 0.0) / PML
    damping = pml_strength * inside * inside * inside / frequency
    factor = 1.0 / (1.0 + damping * damping)
    return factor, -damping * factor


def cmul(a, b):
    return a[0] * b[0] - a[1] * b[1], a[0] * b[1] + a[1] * b[0]


def cadd(a, b):
    return a[0] + b[0], a[1] + b[1]


def csub(a, b):
    return a[0] - b[0], a[1] - b[1]


def cdiv(a, b):
    modulus = b[0] * b[0] + b[1] * b[1]
    return (a[0] * b[0] + a[1] * b[1]) / modulus, (a[1] * b[0] - a[0] * b[1]) / modulus


def kernel(sizes, src, eps, freq, x_out, r_out, V, mat, H, recv_e, recv_p, send_p, recv_yd,
           recv_yu, send_yd, send_yu, recv_dd, recv_du, send_dd, send_du, hrow, fxt, bxt, fyt,
           byt, fym, fzt, bzt, gram, send_g, recv_g, coef, send_sem, recv_sem, gsend_sem,
           grecv_sem, local_sem):
    gx_n, gy_n = sizes
    X, Y, Z = V.shape[3:]
    gx, gy = lax.axis_index("gx"), lax.axis_index("gy")
    frequency = freq[0]
    first_x, last_x = gx == 0, gx == gx_n - 1
    first_y, last_y = gy == 0, gy == gy_n - 1
    devices = gx_n * gy_n
    me = gx * gy_n + gy

    load_src = pltpu.make_async_copy(src, V.at[0], local_sem.at[0])
    load_eps = pltpu.make_async_copy(eps, mat, local_sem.at[1])
    load_src.start()
    load_eps.start()

    barrier = pltpu.get_barrier_semaphore()

    def greet(d, carry):
        other = lax.rem(me + d, devices)
        pl.semaphore_signal(
            barrier, inc=1, device_id={"gx": other // gy_n, "gy": lax.rem(other, gy_n)},
            device_id_type=pl.DeviceIdType.MESH)
        return carry

    lax.fori_loop(1, devices, greet, 0)

    def fill(ref, pair):
        ref[0] = pair[0]
        ref[1] = pair[1]

    def iota(shape, dim):
        return lax.broadcasted_iota(jnp.int32, shape, dim)

    rows_x = fxt.shape[1]
    px = (gx * X - 1 + iota((rows_x, Z), 0)).astype(jnp.float32) + 0.5
    front = stretch(px, X * gx_n, frequency)
    keep = jnp.logical_or(iota((rows_x, Z), 0) > 0, jnp.full((rows_x, Z), gx, jnp.int32) > 0)
    fill(fxt, [jnp.where(keep, f, 0.0) for f in front])
    px = (gx * X + iota((rows_x, Z), 0)).astype(jnp.float32)
    fill(bxt, stretch(px, X * gx_n, frequency))
    py = (gy * Y + iota((Y, Z), 0)).astype(jnp.float32)
    fill(fyt, stretch(py + 0.5, Y * gy_n, frequency))
    fill(byt, stretch(py, Y * gy_n, frequency))
    pm = (gy * Y - 1 + iota((8, Z), 0)).astype(jnp.float32) + 0.5
    keep = jnp.full((8, Z), gy, jnp.int32) > 0
    fill(fym, [jnp.where(keep, f, 0.0) for f in stretch(pm, Y * gy_n, frequency)])
    pz = iota((8, Z), 1).astype(jnp.float32)
    fill(fzt, stretch(pz + 0.5, Z, frequency))
    fill(bzt, stretch(pz, Z, frequency))

    @pl.when(last_x)
    def _():
        recv_e[...] = jnp.zeros_like(recv_e)

    @pl.when(first_x)
    def _():
        recv_p[...] = jnp.zeros_like(recv_p)

    @pl.when(last_y)
    def _():
        recv_yd[...] = jnp.zeros_like(recv_yd)

    @pl.when(first_y)
    def _():
        recv_yu[...] = jnp.zeros_like(recv_yu)

    @pl.when(jnp.logical_or(last_x, first_y))
    def _():
        recv_dd[...] = jnp.zeros_like(recv_dd)

    @pl.when(jnp.logical_or(first_x, last_y))
    def _():
        recv_du[...] = jnp.zeros_like(recv_du)

    gram[...] = jnp.zeros_like(gram)

    def copy(kind, k, source, target, dx, dy):
        return pltpu.make_async_remote_copy(
            src_ref=source, dst_ref=target, send_sem=send_sem.at[kind, k],
            recv_sem=recv_sem.at[kind, k], device_id={"gx": gx + dx, "gy": gy + dy},
            device_id_type=pl.DeviceIdType.MESH)

    def messages(k):
        return {
            DOWN: (lambda: copy(DOWN, k, V.at[k, 1:3, :, 0], recv_e.at[k], -1, 0),
                   gx > 0, gx < gx_n - 1),
            UP: (lambda: copy(UP, k, send_p.at[k], recv_p.at[k], 1, 0),
                 gx < gx_n - 1, gx > 0),
            Y_DOWN: (lambda: copy(Y_DOWN, k, send_yd.at[k], recv_yd.at[k], 0, -1),
                     gy > 0, gy < gy_n - 1),
            Y_UP: (lambda: copy(Y_UP, k, send_yu.at[k], recv_yu.at[k], 0, 1),
                   gy < gy_n - 1, gy > 0),
            DIAG_DOWN: (lambda: copy(DIAG_DOWN, k, send_dd.at[k], recv_dd.at[k], -1, 1),
                        jnp.logical_and(gx > 0, gy < gy_n - 1),
                        jnp.logical_and(gx < gx_n - 1, gy > 0)),
            DIAG_UP: (lambda: copy(DIAG_UP, k, send_du.at[k], recv_du.at[k], 1, -1),
                      jnp.logical_and(gx < gx_n - 1, gy > 0),
                      jnp.logical_and(gx > 0, gy < gy_n - 1)),
        }

    def send(k, kind):
        message, sends, _ = messages(k)[kind]
        pl.when(sends)(lambda: message().start())

    def receive(k, kind):
        message, _, receives = messages(k)[kind]
        pl.when(receives)(lambda: message().wait_recv())

    def row(ref, index):
        return ref[0, pl.ds(index, 1)], ref[1, pl.ds(index, 1)]

    def whole(ref):
        return ref[0], ref[1]

    def next_z(values):
        rolled = pltpu.roll(values, Z - 1, 1)
        return jnp.where(iota(values.shape, 1) == Z - 1, 0.0, rolled)

    def prev_z(values):
        rolled = pltpu.roll(values, 1, 1)
        return jnp.where(iota(values.shape, 1) == 0, 0.0, rolled)

    def next_y(values, edge):
        rolled = pltpu.roll(values, Y - 1, 0)
        return jnp.where(iota(values.shape, 0) == Y - 1, edge, rolled)

    def prev_y(values, edge):
        rolled = pltpu.roll(values, 1, 0)
        return jnp.where(iota(values.shape, 0) == 0, edge, rolled)

    def both(f, *pairs):
        return tuple(f(*[p[i] for p in pairs]) for i in range(2))

    def front_dz(pair):
        return cmul(both(lambda a: next_z(a) - a, pair), row(fzt, 0))

    def back_dz(pair):
        return cmul(both(lambda a: a - prev_z(a), pair), row(bzt, 0))

    def cell(k, component, x):
        return V[k, component, 0, x], V[k, component, 1, x]

    def cells_at(k, component, y):
        return V[k, component, 0, :, y, :], V[k, component, 1, :, y, :]

    zero_row = jnp.zeros((1, Z), jnp.float32)

    def dots(k, layers, first=True):
        def one(j, carry):
            re = jnp.zeros((Y, Z), jnp.float32)
            im = jnp.zeros((Y, Z), jnp.float32)
            for component in range(3):
                for x in layers:
                    a, b = cell(j, component, x), cell(k, component, x)
                    re = re + (a[0] * b[0] + a[1] * b[1])
                    im = im + (a[0] * b[1] - a[1] * b[0])

            def fold(values):
                values = jnp.sum(values, axis=0, keepdims=True)
                return sum(values[:, i:i + LANES] for i in range(0, Z, LANES))

            re, im = fold(re), fold(im)
            if not first:
                re = re + gram[pl.ds(j * SLOTS + k, 1)]
                im = im + gram[pl.ds((SLOTS + j) * SLOTS + k, 1)]
            gram[pl.ds(j * SLOTS + k, 1)] = re
            gram[pl.ds(k * SLOTS + j, 1)] = re
            gram[pl.ds((SLOTS + j) * SLOTS + k, 1)] = im
            gram[pl.ds((SLOTS + k) * SLOTS + j, 1)] = -im
            return carry

        lax.fori_loop(0, k + 1, one, 0)

    def h_layer(k, x, above_y, above_z):
        ex, ey, ez = cell(k, 0, x), cell(k, 1, x), cell(k, 2, x)
        fx, fy = row(fxt, x + 1), whole(fyt)
        ez_edge = recv_yd[k, 1, 0, pl.ds(x, 1)], recv_yd[k, 1, 1, pl.ds(x, 1)]
        ex_edge = recv_yd[k, 0, 0, pl.ds(x, 1)], recv_yd[k, 0, 1, pl.ds(x, 1)]

        def dy(pair, edge):
            return cmul(both(lambda a, e: next_y(a, e) - a, pair, edge), fy)

        hx = csub(dy(ez, ez_edge), front_dz(ey))
        hy = csub(front_dz(ex), cmul(csub(above_z, ez), fx))
        hz = csub(cmul(csub(above_y, ey), fx), dy(ex, ex_edge))
        for component, pair in enumerate((hx, hy, hz)):
            for part in range(2):
                H[component, part, x] = pair[part]

    def hcell(component, x):
        return H[component, 0, x], H[component, 1, x]

    def out_layer(k, x, below_y, below_z, a_k, b_k):
        hx, hy, hz = hcell(0, x), hcell(1, x), hcell(2, x)
        bx, by = row(bxt, x), whole(byt)
        hx_edge = hrow[0, 0, pl.ds(x, 1)], hrow[0, 1, pl.ds(x, 1)]
        hz_edge = hrow[1, 0, pl.ds(x, 1)], hrow[1, 1, pl.ds(x, 1)]

        def dy(pair, edge):
            return cmul(both(lambda a, e: a - prev_y(a, e), pair, edge), by)

        cx = csub(dy(hz, hz_edge), back_dz(hy))
        cy = csub(back_dz(hx), cmul(csub(hz, below_z), bx))
        cz = csub(cmul(csub(hy, below_y), bx), dy(hx, hx_edge))
        before = jnp.maximum(k - 1, 0)
        for component, pair in enumerate((cx, cy, cz)):
            material = mat[component, x]
            for part in range(2):
                value = a_k * (pair[part] - material * V[k, component, part, x])
                V[k + 1, component, part, x] = value - b_k * V[before, component, part, x]

    top = X - 1

    def send_down(k):
        for part in range(2):
            send_dd[k, pl.ds(part, 1)] = V[k, 1, part, 0, pl.ds(Y - 1, 1)]
        send(k, DIAG_DOWN)
        send(k, DOWN)

    def send_up(k):
        for part in range(2):
            send_du[k, pl.ds(part, 1)] = V[k, 0, part, top, pl.ds(0, 1)]
        send(k, DIAG_UP)
        ex, ey, ez = cell(k, 0, top), cell(k, 1, top), cell(k, 2, top)
        fx = row(fxt, X)
        py_ = cadd(front_dz(ex), cmul(ez, fx))
        dy = cmul(both(lambda a: next_y(a, zero_row) - a, ex), whole(fyt))
        pz_ = cadd(cmul(ey, fx), dy)
        for part in range(2):
            send_p[k, 0, part] = py_[part]
            send_p[k, 1, part] = -pz_[part]
        send(k, UP)

    def send_rows(k):
        for part in range(2):
            for i, component in enumerate((0, 2)):
                for x in range(X):
                    send_yd[k, i, part, pl.ds(x, 1)] = V[k, component, part, x, pl.ds(0, 1)]
        send(k, Y_DOWN)
        fy = row(fyt, Y - 1)
        for x in range(X):
            at = pl.ds(Y - 1, 1)
            ex, ey, ez = ((V[k, c, 0, x, at], V[k, c, 1, x, at]) for c in range(3))
            if x < top:
                ahead = V[k, 1, 0, x + 1, at], V[k, 1, 1, x + 1, at]
            else:
                ahead = zero_row, zero_row
            qx = cadd(cmul(ez, fy), front_dz(ey))
            qz = cadd(cmul(csub(ahead, ey), row(fxt, x + 1)), cmul(ex, fy))
            for part in range(2):
                send_yu[k, 0, part, pl.ds(x, 1)] = -qx[part]
                send_yu[k, 1, part, pl.ds(x, 1)] = qz[part]
        send(k, Y_UP)

    def step(k, down_first, last):
        a_k = jnp.where(k == 0, 1.0 / HALF, 2.0 / HALF).astype(jnp.float32)
        b_k = jnp.where(k == 0, 0.0, 1.0).astype(jnp.float32)
        send_rows(k)

        receive(k, Y_DOWN)
        for x in range(X - 1):
            h_layer(k, x, cell(k, 1, x + 1), cell(k, 2, x + 1))

        receive(k, Y_UP)
        fm = row(fym, 0)
        for x in range(X):
            at = pl.ds(0, 1)
            ex, ez = ((V[k, c, 0, x, at], V[k, c, 1, x, at]) for c in (0, 2))
            qx = recv_yu[k, 0, 0, pl.ds(x, 1)], recv_yu[k, 0, 1, pl.ds(x, 1)]
            qz = recv_yu[k, 1, 0, pl.ds(x, 1)], recv_yu[k, 1, 1, pl.ds(x, 1)]
            hx, hz = cadd(qx, cmul(ez, fm)), csub(qz, cmul(ex, fm))
            for part in range(2):
                hrow[0, part, pl.ds(x, 1)] = hx[part]
                hrow[1, part, pl.ds(x, 1)] = hz[part]
        for x in range(1, X - 1):
            out_layer(k, x, hcell(1, x - 1), hcell(2, x - 1), a_k, b_k)

        def from_above():
            receive(k, DIAG_DOWN)
            fix = cmul((recv_dd[k, pl.ds(0, 1)], recv_dd[k, pl.ds(1, 1)]), row(fxt, X))
            for part in range(2):
                hrow[1, part, pl.ds(top, 1)] = hrow[1, part, pl.ds(top, 1)] + fix[part]
            receive(k, DOWN)
            h_layer(k, top, (recv_e[k, 0, 0], recv_e[k, 0, 1]),
                    (recv_e[k, 1, 0], recv_e[k, 1, 1]))
            out_layer(k, top, hcell(1, top - 1), hcell(2, top - 1), a_k, b_k)
            if not last:
                send_up(k + 1)

        def from_below():
            receive(k, DIAG_UP)
            receive(k, UP)
            fx = row(fxt, 0)
            hy = csub((recv_p[k, 0, 0], recv_p[k, 0, 1]), cmul(cell(k, 2, 0), fx))
            hz = cadd((recv_p[k, 1, 0], recv_p[k, 1, 1]), cmul(cell(k, 1, 0), fx))
            fix = cmul((recv_du[k, pl.ds(0, 1)], recv_du[k, pl.ds(1, 1)]), row(fyt, Y - 1))
            hz = both(lambda a, f: jnp.where(iota((Y, Z), 0) == Y - 1, a - f, a), hz, fix)
            out_layer(k, 0, hy, hz, a_k, b_k)
            if not last:
                send_down(k + 1)

        halves = [from_above, from_below]
        if not down_first:
            halves.reverse()
        dots(k, range(X))
        if last:
            dots(k + 1, range(1, X - 1))
        halves[0]()
        halves[1]()
        if last:
            dots(k + 1, sorted({0, top}), first=X < 3)

    def two_steps(pair, carry):
        step(2 * pair, True, False)
        step(2 * pair + 1, True, False)
        return carry

    load_eps.wait()
    square = frequency * frequency
    for component in range(3):
        for x in range(X):
            mat[component, x] = mat[component, x] * square + CENTRE
    load_src.wait()
    pl.semaphore_wait(barrier, devices - 1)

    send_down(0)
    send_up(0)
    lax.fori_loop(0, STEPS // 2 - 1, two_steps, 0)
    step(jnp.int32(STEPS - 2), True, False)
    step(jnp.int32(STEPS - 1), True, True)

    sums = jnp.sum(gram[...], axis=1, keepdims=True)
    count = 2 * SLOTS * SLOTS
    spread = jnp.where(iota((count, LANES), 0) == iota((count, LANES), 1), sums, 0.0)
    send_g[...] = jnp.sum(spread, axis=0, keepdims=True)
    recv_g[me] = send_g[...]

    def gram_copy(d, slot):
        other = lax.rem(me + d, devices)
        return pltpu.make_async_remote_copy(
            src_ref=send_g, dst_ref=recv_g.at[slot], send_sem=gsend_sem.at[d],
            recv_sem=grecv_sem.at[slot],
            device_id={"gx": other // gy_n, "gy": lax.rem(other, gy_n)},
            device_id_type=pl.DeviceIdType.MESH)

    def start(d, carry):
        gram_copy(d, me).start()
        return carry

    lax.fori_loop(1, devices, start, 0)

    def finish(d, carry):
        gram_copy(d, lax.rem(me + d, devices)).wait_recv()
        return carry

    lax.fori_loop(1, devices, finish, 0)
    total = jnp.broadcast_to(jnp.sum(recv_g[...], axis=0), (SLOTS, LANES))

    tile = (SLOTS, LANES)
    sub, lane = iota(tile, 0), iota(tile, 1)

    def unpack(start_at):
        out = jnp.zeros(tile, jnp.float32)
        for i in range(SLOTS):
            shift = (LANES - start_at - i * SLOTS) % LANES
            moved = total if shift == 0 else pltpu.roll(total, shift, 1)
            out = jnp.where(sub == i, moved, out)
        return jnp.where(lane < SLOTS, out, 0.0)

    g = unpack(0), unpack(SLOTS * SLOTS)

    def combine(f, *vectors):
        return tuple(f(*[v[i] for v in vectors]) for i in range(2))

    def operate(vector):
        def one(axis, index, size):
            lift = jnp.where(index == 1, 1.0, jnp.where(index == 0, 0.0, 0.5))
            drop = jnp.where(index < SLOTS - 1, 0.5, 0.0)

            def real(p):
                moved = lift * pltpu.roll(p, 1, axis) + drop * pltpu.roll(p, size - 1, axis)
                return CENTRE * p + HALF * moved
            return real

        along, down = vector
        return (both(one(1, lane, LANES), along), both(one(0, sub, SLOTS), down))

    def inner(left, right):
        t = cmul(g, right[0])
        a = left[1]

        def full(values):
            return jnp.sum(jnp.sum(values, axis=1, keepdims=True), axis=0, keepdims=True)

        return full(a[0] * t[0] + a[1] * t[1]), full(a[0] * t[1] - a[1] * t[0])

    def scaled(vector, number):
        return combine(lambda v: cmul(v, number), vector)

    zero = jnp.zeros(tile, jnp.float32)
    unit = ((jnp.where(lane == 0, 1.0, 0.0), zero), (jnp.where(sub == 0, 1.0, 0.0), zero))
    answer = ((zero, zero), (zero, zero))
    residual = direction = unit
    rho = inner(unit, unit)
    for iteration in range(ITERS):
        image = operate(direction)
        alpha = cdiv(rho, inner(unit, image))
        middle = combine(csub, residual, scaled(image, alpha))
        second = operate(middle)
        weight = cdiv(inner(second, middle), inner(second, second))
        answer = combine(cadd, answer, scaled(direction, alpha))
        answer = combine(cadd, answer, scaled(middle, weight))
        residual = combine(csub, middle, scaled(second, weight))
        if iteration + 1 < ITERS:
            moved = cmul(weight, inner(unit, second))
            rho_next = -moved[0], -moved[1]
            beta = cmul(cdiv(rho_next, rho), cdiv(alpha, weight))
            pull = combine(csub, direction, scaled(image, weight))
            direction = combine(cadd, residual, scaled(pull, beta))
            rho = rho_next

    for i, values in enumerate((answer[1][0], answer[1][1], residual[1][0], residual[1][1])):
        for at in range(0, Z, LANES):
            coef[i, :, pl.ds(at, LANES)] = values

    chunk = 16 if Y % 16 == 0 else 8

    def emit(index, carry):
        at = pl.ds(pl.multiple_of(lax.rem(index, Y // chunk) * chunk, 8), chunk)
        index = index // (Y // chunk)
        component, x = index // X, lax.rem(index, X)
        sums = [jnp.zeros((chunk, Z), jnp.float32)] * 4
        for k in range(STEPS + 1):
            v = V[k, component, 0, x, at], V[k, component, 1, x, at]
            for base in ((0, 2) if k < STEPS else (2,)):
                p = cmul(v, (coef[base, pl.ds(k, 1)], coef[base + 1, pl.ds(k, 1)]))
                sums[base], sums[base + 1] = sums[base] + p[0], sums[base + 1] + p[1]
        for part in range(2):
            x_out[component, part, x, at] = sums[part]
            r_out[component, part, x, at] = sums[2 + part]
        return carry

    lax.fori_loop(0, 3 * X * (Y // chunk), emit, 0)

    def drain(k, carry):
        for message, sends, _ in messages(k).values():
            pl.when(sends)(lambda: message().wait_send())
        return carry

    lax.fori_loop(0, STEPS, drain, 0)

    def drain_gram(d, carry):
        gram_copy(d, me).wait_send()
        return carry

    lax.fori_loop(1, devices, drain_gram, 0)


def solution(mesh):
    gx_n, gy_n = mesh.shape["gx"], mesh.shape["gy"]
    devices = gx_n * gy_n

    def body(source, permittivity, frequency):
        X, Y, Z = source.shape[3:]
        field = source.shape[1:]
        f32 = jnp.float32
        rows_x = -(-(X + 1) // 8) * 8
        vmem = pltpu.VMEM
        face = (STEPS, 2, 2, Y, Z)
        rows = (STEPS, 2, 2, X, Z)
        diag = (STEPS, 2, Z)
        scratch = [
            vmem((STEPS + 1,) + field, f32), vmem(permittivity.shape, f32), vmem(field, f32),
            vmem(face, f32), vmem(face, f32), vmem(face, f32),
            vmem(rows, f32), vmem(rows, f32), vmem(rows, f32), vmem(rows, f32),
            vmem(diag, f32), vmem(diag, f32), vmem(diag, f32), vmem(diag, f32),
            vmem(rows[1:], f32),
            vmem((2, rows_x, Z), f32), vmem((2, rows_x, Z), f32),
            vmem((2, Y, Z), f32), vmem((2, Y, Z), f32), vmem((2, 8, Z), f32),
            vmem((2, 8, Z), f32), vmem((2, 8, Z), f32),
            vmem((2 * SLOTS * SLOTS, LANES), f32), vmem((1, LANES), f32),
            vmem((devices, 1, LANES), f32), vmem((4, SLOTS, Z), f32),
            pltpu.SemaphoreType.DMA((6, STEPS)), pltpu.SemaphoreType.DMA((6, STEPS)),
            pltpu.SemaphoreType.DMA((devices,)), pltpu.SemaphoreType.DMA((devices,)),
            pltpu.SemaphoreType.DMA((2,)),
        ]
        out = pl.pallas_call(
            functools.partial(kernel, (gx_n, gy_n)),
            out_shape=(jax.ShapeDtypeStruct(field, f32),) * 2,
            in_specs=[pl.BlockSpec(memory_space=pltpu.HBM), pl.BlockSpec(memory_space=pltpu.HBM),
                      pl.BlockSpec(memory_space=pltpu.SMEM)],
            out_specs=(pl.BlockSpec(memory_space=vmem),) * 2,
            scratch_shapes=scratch,
            compiler_params=pltpu.CompilerParams(
                collective_id=0, has_side_effects=True, vmem_limit_bytes=48 * 1024 * 1024),
        )(source[0], permittivity, frequency)
        return out[0][None], out[1][None]

    placed = (P("groups", None, None, "gx", "gy", None), P("groups", "gx", "gy", None), P())
    return jax.shard_map(
        body,
        mesh=mesh,
        in_specs=placed,
        out_specs=(
            P("groups", None, None, "gx", "gy", None),
            P("groups", None, None, "gx", "gy", None),
        ),
        check_vma=False,
    )
```

```python
import functools

import jax
import jax.numpy as jnp
from jax import lax
from jax.experimental import pallas as pl
from jax.experimental.pallas import tpu as pltpu
from jax.sharding import PartitionSpec as P

PML = 8
ITERS = 3
STEPS = 2 * ITERS
SLOTS = 8
CENTRE = 4.0
HALF = 8.0
LANES = 128
pml_strength = 2.0

DOWN, UP, Y_DOWN, Y_UP, DIAG_DOWN, DIAG_UP = range(6)


def stretch(points, length, frequency):
    inside = jnp.maximum(jnp.maximum(PML - points, points - (length - PML)), 0.0) / PML
    damping = pml_strength * inside * inside * inside / frequency
    factor = 1.0 / (1.0 + damping * damping)
    return factor, -damping * factor


def cmul(a, b):
    return a[0] * b[0] - a[1] * b[1], a[0] * b[1] + a[1] * b[0]


def cadd(a, b):
    return a[0] + b[0], a[1] + b[1]


def csub(a, b):
    return a[0] - b[0], a[1] - b[1]


def cdiv(a, b):
    modulus = b[0] * b[0] + b[1] * b[1]
    return (a[0] * b[0] + a[1] * b[1]) / modulus, (a[1] * b[0] - a[0] * b[1]) / modulus


def kernel(sizes, src, eps, freq, x_out, r_out, V, mat, H, recv_e, recv_p, send_p, recv_yd,
           recv_yu, send_yd, send_yu, recv_dd, recv_du, send_dd, send_du, hrow, fxt, bxt, fyt,
           byt, fym, fzt, bzt, gram, send_g, recv_g, coef, send_sem, recv_sem, gsend_sem,
           grecv_sem, local_sem):
    gx_n, gy_n = sizes
    X, Y, Z = V.shape[3:]
    gx, gy = lax.axis_index("gx"), lax.axis_index("gy")
    frequency = freq[0]
    first_x, last_x = gx == 0, gx == gx_n - 1
    first_y, last_y = gy == 0, gy == gy_n - 1
    devices = gx_n * gy_n
    me = gx * gy_n + gy

    load_src = pltpu.make_async_copy(src, V.at[0], local_sem.at[0])
    load_eps = pltpu.make_async_copy(eps, mat, local_sem.at[1])
    load_src.start()
    load_eps.start()

    barrier = pltpu.get_barrier_semaphore()

    def greet(d, carry):
        other = lax.rem(me + d, devices)
        pl.semaphore_signal(
            barrier, inc=1, device_id={"gx": other // gy_n, "gy": lax.rem(other, gy_n)},
            device_id_type=pl.DeviceIdType.MESH)
        return carry

    lax.fori_loop(1, devices, greet, 0)

    def fill(ref, pair):
        ref[0] = pair[0]
        ref[1] = pair[1]

    def iota(shape, dim):
        return lax.broadcasted_iota(jnp.int32, shape, dim)

    rows_x = fxt.shape[1]
    px = (gx * X - 1 + iota((rows_x, Z), 0)).astype(jnp.float32) + 0.5
    front = stretch(px, X * gx_n, frequency)
    keep = jnp.logical_or(iota((rows_x, Z), 0) > 0, jnp.full((rows_x, Z), gx, jnp.int32) > 0)
    fill(fxt, [jnp.where(keep, f, 0.0) for f in front])
    px = (gx * X + iota((rows_x, Z), 0)).astype(jnp.float32)
    fill(bxt, stretch(px, X * gx_n, frequency))
    py = (gy * Y + iota((Y, Z), 0)).astype(jnp.float32)
    fill(fyt, stretch(py + 0.5, Y * gy_n, frequency))
    fill(byt, stretch(py, Y * gy_n, frequency))
    pm = (gy * Y - 1 + iota((8, Z), 0)).astype(jnp.float32) + 0.5
    keep = jnp.full((8, Z), gy, jnp.int32) > 0
    fill(fym, [jnp.where(keep, f, 0.0) for f in stretch(pm, Y * gy_n, frequency)])
    pz = iota((8, Z), 1).astype(jnp.float32)
    fill(fzt, stretch(pz + 0.5, Z, frequency))
    fill(bzt, stretch(pz, Z, frequency))

    @pl.when(last_x)
    def _():
        recv_e[...] = jnp.zeros_like(recv_e)

    @pl.when(first_x)
    def _():
        recv_p[...] = jnp.zeros_like(recv_p)

    @pl.when(last_y)
    def _():
        recv_yd[...] = jnp.zeros_like(recv_yd)

    @pl.when(first_y)
    def _():
        recv_yu[...] = jnp.zeros_like(recv_yu)

    @pl.when(jnp.logical_or(last_x, first_y))
    def _():
        recv_dd[...] = jnp.zeros_like(recv_dd)

    @pl.when(jnp.logical_or(first_x, last_y))
    def _():
        recv_du[...] = jnp.zeros_like(recv_du)

    gram[...] = jnp.zeros_like(gram)

    def copy(kind, k, source, target, dx, dy):
        return pltpu.make_async_remote_copy(
            src_ref=source, dst_ref=target, send_sem=send_sem.at[kind, k],
            recv_sem=recv_sem.at[kind, k], device_id={"gx": gx + dx, "gy": gy + dy},
            device_id_type=pl.DeviceIdType.MESH)

    def messages(k):
        return {
            DOWN: (lambda: copy(DOWN, k, V.at[k, 1:3, :, 0], recv_e.at[k], -1, 0),
                   gx > 0, gx < gx_n - 1),
            UP: (lambda: copy(UP, k, send_p.at[k], recv_p.at[k], 1, 0),
                 gx < gx_n - 1, gx > 0),
            Y_DOWN: (lambda: copy(Y_DOWN, k, send_yd.at[k], recv_yd.at[k], 0, -1),
                     gy > 0, gy < gy_n - 1),
            Y_UP: (lambda: copy(Y_UP, k, send_yu.at[k], recv_yu.at[k], 0, 1),
                   gy < gy_n - 1, gy > 0),
            DIAG_DOWN: (lambda: copy(DIAG_DOWN, k, send_dd.at[k], recv_dd.at[k], -1, 1),
                        jnp.logical_and(gx > 0, gy < gy_n - 1),
                        jnp.logical_and(gx < gx_n - 1, gy > 0)),
            DIAG_UP: (lambda: copy(DIAG_UP, k, send_du.at[k], recv_du.at[k], 1, -1),
                      jnp.logical_and(gx < gx_n - 1, gy > 0),
                      jnp.logical_and(gx > 0, gy < gy_n - 1)),
        }

    def send(k, kind):
        message, sends, _ = messages(k)[kind]
        pl.when(sends)(lambda: message().start())

    def receive(k, kind):
        message, _, receives = messages(k)[kind]
        pl.when(receives)(lambda: message().wait_recv())

    def row(ref, index):
        return ref[0, pl.ds(index, 1)], ref[1, pl.ds(index, 1)]

    def whole(ref):
        return ref[0], ref[1]

    def next_z(values):
        rolled = pltpu.roll(values, Z - 1, 1)
        return jnp.where(iota(values.shape, 1) == Z - 1, 0.0, rolled)

    def prev_z(values):
        rolled = pltpu.roll(values, 1, 1)
        return jnp.where(iota(values.shape, 1) == 0, 0.0, rolled)

    def next_y(values, edge):
        rolled = pltpu.roll(values, Y - 1, 0)
        return jnp.where(iota(values.shape, 0) == Y - 1, edge, rolled)

    def prev_y(values, edge):
        rolled = pltpu.roll(values, 1, 0)
        return jnp.where(iota(values.shape, 0) == 0, edge, rolled)

    def both(f, *pairs):
        return tuple(f(*[p[i] for p in pairs]) for i in range(2))

    def front_dz(pair):
        return cmul(both(lambda a: next_z(a) - a, pair), row(fzt, 0))

    def back_dz(pair):
        return cmul(both(lambda a: a - prev_z(a), pair), row(bzt, 0))

    def cell(k, component, x):
        return V[k, component, 0, x], V[k, component, 1, x]

    def cells_at(k, component, y):
        return V[k, component, 0, :, y, :], V[k, component, 1, :, y, :]

    zero_row = jnp.zeros((1, Z), jnp.float32)

    def dots(k, layers, first=True):
        def one(j, carry):
            re = jnp.zeros((Y, Z), jnp.float32)
            im = jnp.zeros((Y, Z), jnp.float32)
            for component in range(3):
                for x in layers:
                    a, b = cell(j, component, x), cell(k, component, x)
                    re = re + (a[0] * b[0] + a[1] * b[1])
                    im = im + (a[0] * b[1] - a[1] * b[0])

            def fold(values):
                values = jnp.sum(values, axis=0, keepdims=True)
                return sum(values[:, i:i + LANES] for i in range(0, Z, LANES))

            re, im = fold(re), fold(im)
            if not first:
                re = re + gram[pl.ds(j * SLOTS + k, 1)]
                im = im + gram[pl.ds((SLOTS + j) * SLOTS + k, 1)]
            gram[pl.ds(j * SLOTS + k, 1)] = re
            gram[pl.ds(k * SLOTS + j, 1)] = re
            gram[pl.ds((SLOTS + j) * SLOTS + k, 1)] = im
            gram[pl.ds((SLOTS + k) * SLOTS + j, 1)] = -im
            return carry

        lax.fori_loop(0, k + 1, one, 0)

    def h_layer(k, x, above_y, above_z):
        ex, ey, ez = cell(k, 0, x), cell(k, 1, x), cell(k, 2, x)
        fx, fy = row(fxt, x + 1), whole(fyt)
        ez_edge = recv_yd[k, 1, 0, pl.ds(x, 1)], recv_yd[k, 1, 1, pl.ds(x, 1)]
        ex_edge = recv_yd[k, 0, 0, pl.ds(x, 1)], recv_yd[k, 0, 1, pl.ds(x, 1)]

        def dy(pair, edge):
            return cmul(both(lambda a, e: next_y(a, e) - a, pair, edge), fy)

        hx = csub(dy(ez, ez_edge), front_dz(ey))
        hy = csub(front_dz(ex), cmul(csub(above_z, ez), fx))
        hz = csub(cmul(csub(above_y, ey), fx), dy(ex, ex_edge))
        for component, pair in enumerate((hx, hy, hz)):
            for part in range(2):
                H[component, part, x] = pair[part]

    def hcell(component, x):
        return H[component, 0, x], H[component, 1, x]

    def out_layer(k, x, below_y, below_z, a_k, b_k):
        hx, hy, hz = hcell(0, x), hcell(1, x), hcell(2, x)
        bx, by = row(bxt, x), whole(byt)
        hx_edge = hrow[0, 0, pl.ds(x, 1)], hrow[0, 1, pl.ds(x, 1)]
        hz_edge = hrow[1, 0, pl.ds(x, 1)], hrow[1, 1, pl.ds(x, 1)]

        def dy(pair, edge):
            return cmul(both(lambda a, e: a - prev_y(a, e), pair, edge), by)

        cx = csub(dy(hz, hz_edge), back_dz(hy))
        cy = csub(back_dz(hx), cmul(csub(hz, below_z), bx))
        cz = csub(cmul(csub(hy, below_y), bx), dy(hx, hx_edge))
        before = jnp.maximum(k - 1, 0)
        for component, pair in enumerate((cx, cy, cz)):
            material = mat[component, x]
            for part in range(2):
                value = a_k * (pair[part] - material * V[k, component, part, x])
                V[k + 1, component, part, x] = value - b_k * V[before, component, part, x]

    top = X - 1

    def send_down(k):
        for part in range(2):
            send_dd[k, pl.ds(part, 1)] = V[k, 1, part, 0, pl.ds(Y - 1, 1)]
        send(k, DIAG_DOWN)
        send(k, DOWN)

    def send_up(k):
        for part in range(2):
            send_du[k, pl.ds(part, 1)] = V[k, 0, part, top, pl.ds(0, 1)]
        send(k, DIAG_UP)
        ex, ey, ez = cell(k, 0, top), cell(k, 1, top), cell(k, 2, top)
        fx = row(fxt, X)
        py_ = cadd(front_dz(ex), cmul(ez, fx))
        dy = cmul(both(lambda a: next_y(a, zero_row) - a, ex), whole(fyt))
        pz_ = cadd(cmul(ey, fx), dy)
        for part in range(2):
            send_p[k, 0, part] = py_[part]
            send_p[k, 1, part] = -pz_[part]
        send(k, UP)

    def send_rows(k):
        for part in range(2):
            for i, component in enumerate((0, 2)):
                for x in range(X):
                    send_yd[k, i, part, pl.ds(x, 1)] = V[k, component, part, x, pl.ds(0, 1)]
        send(k, Y_DOWN)
        fy = row(fyt, Y - 1)
        for x in range(X):
            at = pl.ds(Y - 1, 1)
            ex, ey, ez = ((V[k, c, 0, x, at], V[k, c, 1, x, at]) for c in range(3))
            if x < top:
                ahead = V[k, 1, 0, x + 1, at], V[k, 1, 1, x + 1, at]
            else:
                ahead = zero_row, zero_row
            qx = cadd(cmul(ez, fy), front_dz(ey))
            qz = cadd(cmul(csub(ahead, ey), row(fxt, x + 1)), cmul(ex, fy))
            for part in range(2):
                send_yu[k, 0, part, pl.ds(x, 1)] = -qx[part]
                send_yu[k, 1, part, pl.ds(x, 1)] = qz[part]
        send(k, Y_UP)

    def step(k, down_first, last):
        a_k = jnp.where(k == 0, 1.0 / HALF, 2.0 / HALF).astype(jnp.float32)
        b_k = jnp.where(k == 0, 0.0, 1.0).astype(jnp.float32)
        send_rows(k)

        receive(k, Y_DOWN)
        for x in range(X - 1):
            h_layer(k, x, cell(k, 1, x + 1), cell(k, 2, x + 1))

        receive(k, Y_UP)
        fm = row(fym, 0)
        for x in range(X):
            at = pl.ds(0, 1)
            ex, ez = ((V[k, c, 0, x, at], V[k, c, 1, x, at]) for c in (0, 2))
            qx = recv_yu[k, 0, 0, pl.ds(x, 1)], recv_yu[k, 0, 1, pl.ds(x, 1)]
            qz = recv_yu[k, 1, 0, pl.ds(x, 1)], recv_yu[k, 1, 1, pl.ds(x, 1)]
            hx, hz = cadd(qx, cmul(ez, fm)), csub(qz, cmul(ex, fm))
            for part in range(2):
                hrow[0, part, pl.ds(x, 1)] = hx[part]
                hrow[1, part, pl.ds(x, 1)] = hz[part]
        for x in range(1, X - 1):
            out_layer(k, x, hcell(1, x - 1), hcell(2, x - 1), a_k, b_k)

        def from_above():
            receive(k, DIAG_DOWN)
            fix = cmul((recv_dd[k, pl.ds(0, 1)], recv_dd[k, pl.ds(1, 1)]), row(fxt, X))
            for part in range(2):
                hrow[1, part, pl.ds(top, 1)] = hrow[1, part, pl.ds(top, 1)] + fix[part]
            receive(k, DOWN)
            h_layer(k, top, (recv_e[k, 0, 0], recv_e[k, 0, 1]),
                    (recv_e[k, 1, 0], recv_e[k, 1, 1]))
            out_layer(k, top, hcell(1, top - 1), hcell(2, top - 1), a_k, b_k)
            if not last:
                send_up(k + 1)

        def from_below():
            receive(k, DIAG_UP)
            receive(k, UP)
            fx = row(fxt, 0)
            hy = csub((recv_p[k, 0, 0], recv_p[k, 0, 1]), cmul(cell(k, 2, 0), fx))
            hz = cadd((recv_p[k, 1, 0], recv_p[k, 1, 1]), cmul(cell(k, 1, 0), fx))
            fix = cmul((recv_du[k, pl.ds(0, 1)], recv_du[k, pl.ds(1, 1)]), row(fyt, Y - 1))
            hz = both(lambda a, f: jnp.where(iota((Y, Z), 0) == Y - 1, a - f, a), hz, fix)
            out_layer(k, 0, hy, hz, a_k, b_k)
            if not last:
                send_down(k + 1)

        halves = [from_above, from_below]
        if not down_first:
            halves.reverse()
        dots(k, range(X))
        if last:
            dots(k + 1, range(1, X - 1))
        halves[0]()
        halves[1]()
        if last:
            dots(k + 1, sorted({0, top}), first=X < 3)

    def two_steps(pair, carry):
        step(2 * pair, True, False)
        step(2 * pair + 1, True, False)
        return carry

    load_eps.wait()
    square = frequency * frequency
    for component in range(3):
        for x in range(X):
            mat[component, x] = mat[component, x] * square + CENTRE
    load_src.wait()
    pl.semaphore_wait(barrier, devices - 1)

    send_down(0)
    send_up(0)
    lax.fori_loop(0, STEPS // 2 - 1, two_steps, 0)
    step(jnp.int32(STEPS - 2), True, False)
    step(jnp.int32(STEPS - 1), True, True)

    sums = jnp.sum(gram[...], axis=1, keepdims=True)
    count = 2 * SLOTS * SLOTS
    spread = jnp.where(iota((count, LANES), 0) == iota((count, LANES), 1), sums, 0.0)
    send_g[...] = jnp.sum(spread, axis=0, keepdims=True)
    recv_g[me] = send_g[...]

    def gram_copy(d, slot):
        other = lax.rem(me + d, devices)
        return pltpu.make_async_remote_copy(
            src_ref=send_g, dst_ref=recv_g.at[slot], send_sem=gsend_sem.at[d],
            recv_sem=grecv_sem.at[slot],
            device_id={"gx": other // gy_n, "gy": lax.rem(other, gy_n)},
            device_id_type=pl.DeviceIdType.MESH)

    def start(d, carry):
        gram_copy(d, me).start()
        return carry

    lax.fori_loop(1, devices, start, 0)

    def finish(d, carry):
        gram_copy(d, lax.rem(me + d, devices)).wait_recv()
        return carry

    lax.fori_loop(1, devices, finish, 0)
    total = jnp.broadcast_to(jnp.sum(recv_g[...], axis=0), (SLOTS, LANES))

    tile = (SLOTS, LANES)
    sub, lane = iota(tile, 0), iota(tile, 1)

    def unpack(start_at):
        out = jnp.zeros(tile, jnp.float32)
        for i in range(SLOTS):
            shift = (LANES - start_at - i * SLOTS) % LANES
            moved = total if shift == 0 else pltpu.roll(total, shift, 1)
            out = jnp.where(sub == i, moved, out)
        return jnp.where(lane < SLOTS, out, 0.0)

    g = unpack(0), unpack(SLOTS * SLOTS)

    def combine(f, *vectors):
        return tuple(f(*[v[i] for v in vectors]) for i in range(2))

    def operate(vector):
        def one(axis, index, size):
            lift = jnp.where(index == 1, 1.0, jnp.where(index == 0, 0.0, 0.5))
            drop = jnp.where(index < SLOTS - 1, 0.5, 0.0)

            def real(p):
                moved = lift * pltpu.roll(p, 1, axis) + drop * pltpu.roll(p, size - 1, axis)
                return CENTRE * p + HALF * moved
            return real

        along, down = vector
        return (both(one(1, lane, LANES), along), both(one(0, sub, SLOTS), down))

    def inner(left, right):
        t = cmul(g, right[0])
        a = left[1]

        def full(values):
            return jnp.sum(jnp.sum(values, axis=1, keepdims=True), axis=0, keepdims=True)

        return full(a[0] * t[0] + a[1] * t[1]), full(a[0] * t[1] - a[1] * t[0])

    def scaled(vector, number):
        return combine(lambda v: cmul(v, number), vector)

    zero = jnp.zeros(tile, jnp.float32)
    unit = ((jnp.where(lane == 0, 1.0, 0.0), zero), (jnp.where(sub == 0, 1.0, 0.0), zero))
    answer = ((zero, zero), (zero, zero))
    residual = direction = unit
    rho = inner(unit, unit)
    for iteration in range(ITERS):
        image = operate(direction)
        alpha = cdiv(rho, inner(unit, image))
        middle = combine(csub, residual, scaled(image, alpha))
        second = operate(middle)
        weight = cdiv(inner(second, middle), inner(second, second))
        answer = combine(cadd, answer, scaled(direction, alpha))
        answer = combine(cadd, answer, scaled(middle, weight))
        residual = combine(csub, middle, scaled(second, weight))
        if iteration + 1 < ITERS:
            moved = cmul(weight, inner(unit, second))
            rho_next = -moved[0], -moved[1]
            beta = cmul(cdiv(rho_next, rho), cdiv(alpha, weight))
            pull = combine(csub, direction, scaled(image, weight))
            direction = combine(cadd, residual, scaled(pull, beta))
            rho = rho_next

    for i, values in enumerate((answer[1][0], answer[1][1], residual[1][0], residual[1][1])):
        for at in range(0, Z, LANES):
            coef[i, :, pl.ds(at, LANES)] = values

    chunk = 16 if Y % 16 == 0 else 8

    def emit(index, carry):
        at = pl.ds(pl.multiple_of(lax.rem(index, Y // chunk) * chunk, 8), chunk)
        index = index // (Y // chunk)
        component, x = index // X, lax.rem(index, X)
        sums = [jnp.zeros((chunk, Z), jnp.float32)] * 4
        for k in range(STEPS + 1):
            v = V[k, component, 0, x, at], V[k, component, 1, x, at]
            for base in ((0, 2) if k < STEPS else (2,)):
                p = cmul(v, (coef[base, pl.ds(k, 1)], coef[base + 1, pl.ds(k, 1)]))
                sums[base], sums[base + 1] = sums[base] + p[0], sums[base + 1] + p[1]
        for part in range(2):
            x_out[component, part, x, at] = sums[part]
            r_out[component, part, x, at] = sums[2 + part]
        return carry

    lax.fori_loop(0, 3 * X * (Y // chunk), emit, 0)

    def drain(k, carry):
        for message, sends, _ in messages(k).values():
            pl.when(sends)(lambda: message().wait_send())
        return carry

    lax.fori_loop(0, STEPS, drain, 0)

    def drain_gram(d, carry):
        gram_copy(d, me).wait_send()
        return carry

    lax.fori_loop(1, devices, drain_gram, 0)


def solution(mesh):
    gx_n, gy_n = mesh.shape["gx"], mesh.shape["gy"]
    devices = gx_n * gy_n

    def body(source, permittivity, frequency):
        X, Y, Z = source.shape[3:]
        field = source.shape[1:]
        f32 = jnp.float32
        rows_x = -(-(X + 1) // 8) * 8
        vmem = pltpu.VMEM
        face = (STEPS, 2, 2, Y, Z)
        rows = (STEPS, 2, 2, X, Z)
        diag = (STEPS, 2, Z)
        scratch = [
            vmem((STEPS + 1,) + field, f32), vmem(permittivity.shape, f32), vmem(field, f32),
            vmem(face, f32), vmem(face, f32), vmem(face, f32),
            vmem(rows, f32), vmem(rows, f32), vmem(rows, f32), vmem(rows, f32),
            vmem(diag, f32), vmem(diag, f32), vmem(diag, f32), vmem(diag, f32),
            vmem(rows[1:], f32),
            vmem((2, rows_x, Z), f32), vmem((2, rows_x, Z), f32),
            vmem((2, Y, Z), f32), vmem((2, Y, Z), f32), vmem((2, 8, Z), f32),
            vmem((2, 8, Z), f32), vmem((2, 8, Z), f32),
            vmem((2 * SLOTS * SLOTS, LANES), f32), vmem((1, LANES), f32),
            vmem((devices, 1, LANES), f32), vmem((4, SLOTS, Z), f32),
            pltpu.SemaphoreType.DMA((6, STEPS)), pltpu.SemaphoreType.DMA((6, STEPS)),
            pltpu.SemaphoreType.DMA((devices,)), pltpu.SemaphoreType.DMA((devices,)),
            pltpu.SemaphoreType.DMA((2,)),
        ]
        out = pl.pallas_call(
            functools.partial(kernel, (gx_n, gy_n)),
            out_shape=(jax.ShapeDtypeStruct(field, f32),) * 2,
            in_specs=[pl.BlockSpec(memory_space=pltpu.HBM), pl.BlockSpec(memory_space=pltpu.HBM),
                      pl.BlockSpec(memory_space=pltpu.SMEM)],
            out_specs=(pl.BlockSpec(memory_space=vmem),) * 2,
            scratch_shapes=scratch,
            compiler_params=pltpu.CompilerParams(
                collective_id=0, has_side_effects=True, vmem_limit_bytes=48 * 1024 * 1024),
        )(pltpu.with_memory_space_constraint(source[0], pltpu.HBM), pltpu.with_memory_space_constraint(permittivity, pltpu.HBM), frequency)
        return out[0][None], out[1][None]

    placed = (P("groups", None, None, "gx", "gy", None), P("groups", "gx", "gy", None), P())
    return jax.shard_map(
        body,
        mesh=mesh,
        in_specs=placed,
        out_specs=(
            P("groups", None, None, "gx", "gy", None),
            P("groups", None, None, "gx", "gy", None),
        ),
        check_vma=False,
    )
```
